32 devices in a mesh: fsdp: 32 (over z, y, x, core).
Axes of the slice: x: 2, y: 2, z: 4, core: 2. Of those that a mesh axis runs over, the one named last changes fastest.
Arguments:
- resid_in: bfloat16 [256, 257, 1024], P('fsdp')
- grad_out: bfloat16 [256, 257, 1024], P('fsdp')
- ln1_gain: float32 [1024], P('fsdp')
- ln1_bias: float32 [1024], P('fsdp')
- qkv_weight: float32 [1024, 3072], P('fsdp')
- qkv_bias: float32 [3072], P('fsdp')
- out_weight: float32 [1024, 1024], P('fsdp')
- out_bias: float32 [1024], P('fsdp')
- ln2_gain: float32 [1024], P('fsdp')
- ln2_bias: float32 [1024], P('fsdp')
- fc_weight: float32 [1024, 4096], P('fsdp')
- fc_bias: float32 [4096], P('fsdp')
- proj_weight: float32 [4096, 1024], P('fsdp')
- proj_bias: float32 [1024], P('fsdp')
Outputs:
- output 1: bfloat16 [256, 257, 1024], P('fsdp')
- output 2: bfloat16 [256, 257, 1024], P('fsdp')
- output 3: float32 [1024], P('fsdp')
- output 4: float32 [1024], P('fsdp')
- output 5: float32 [1024, 3072], P('fsdp')
- output 6: float32 [3072], P('fsdp')
- output 7: float32 [1024, 1024], P('fsdp')
- output 8: float32 [1024], P('fsdp')
- output 9: float32 [1024], P('fsdp')
- output 10: float32 [1024], P('fsdp')
- output 11: float32 [1024, 4096], P('fsdp')
- output 12: float32 [4096], P('fsdp')
- output 13: float32 [4096, 1024], P('fsdp')
- output 14: float32 [1024], P('fsdp')
All inputs are finite; a program needn't handle non-finite values.
Results may differ from the reference program's by a relative error of at most 0.02.
Values are sent between devices in bfloat16 or wider.
A program may use at most 1 GiB of HBM per device.

```python
import jax
import jax.numpy as jnp
from jax import lax

WIDTH = 1024
FFN = 4096
HEADS = 16
PATCHES = 256
BATCH = 256

SEQ = PATCHES + 1
HEAD_DIM = WIDTH // HEADS
LN_EPS = 1e-5


def setup_inputs(seed: int = 0) -> dict:
    keys = jax.random.split(jax.random.key(seed), 14)

    def normal(key_index, shape, scale):
        return jax.random.normal(keys[key_index], shape, jnp.float32) * scale

    return {
        "resid_in": normal(0, (BATCH, SEQ, WIDTH), 1.0).astype(jnp.bfloat16),
        "grad_out": normal(1, (BATCH, SEQ, WIDTH), 1.0).astype(jnp.bfloat16),
        "ln1_gain": 1.0 + normal(2, (WIDTH,), 0.6),
        "ln1_bias": normal(3, (WIDTH,), 1.0),
        "qkv_weight": normal(4, (WIDTH, 3 * WIDTH), WIDTH ** -0.5),
        "qkv_bias": normal(5, (3 * WIDTH,), 1.0),
        "out_weight": normal(6, (WIDTH, WIDTH), WIDTH ** -0.5),
        "out_bias": normal(7, (WIDTH,), 1.0),
        "ln2_gain": 1.0 + normal(8, (WIDTH,), 0.6),
        "ln2_bias": normal(9, (WIDTH,), 1.0),
        "fc_weight": normal(10, (WIDTH, FFN), WIDTH ** -0.5),
        "fc_bias": normal(11, (FFN,), 1.0),
        "proj_weight": normal(12, (FFN, WIDTH), FFN ** -0.5),
        "proj_bias": normal(13, (WIDTH,), 1.0),
    }


def layer_norm(values, gain, bias):
    mean_val = jnp.mean(values, axis=-1, keepdims=True)
    centered = values - mean_val
    variance = jnp.mean(centered * centered, axis=-1, keepdims=True)
    return centered * lax.rsqrt(variance + LN_EPS) * gain + bias


def layer_forward(params, tokens):
    (ln1_gain, ln1_bias, qkv_weight, qkv_bias, out_weight, out_bias,
     ln2_gain, ln2_bias, fc_weight, fc_bias, proj_weight, proj_bias) = [param.astype(jnp.bfloat16) for param in params]
    resid = tokens.astype(jnp.float32)
    normed_one = layer_norm(resid, ln1_gain, ln1_bias).astype(jnp.bfloat16)
    qkv_vals = (jnp.dot(normed_one, qkv_weight, preferred_element_type=jnp.float32) + qkv_bias).astype(jnp.bfloat16)
    qkv_vals = qkv_vals.reshape(SEQ, 3, HEADS, HEAD_DIM).astype(jnp.float32)
    scores = jnp.einsum("qhd,khd->hqk", qkv_vals[:, 0], qkv_vals[:, 1]) * (HEAD_DIM ** -0.5)
    attn_probs = jax.nn.softmax(scores, axis=-1).astype(jnp.bfloat16).astype(jnp.float32)
    mixed = jnp.einsum("hqk,khd->qhd", attn_probs, qkv_vals[:, 2]).astype(jnp.bfloat16).reshape(SEQ, WIDTH)
    middle = (resid + jnp.dot(mixed, out_weight, preferred_element_type=jnp.float32) + out_bias).astype(jnp.bfloat16)
    middle_wide = middle.astype(jnp.float32)
    normed_two = layer_norm(middle_wide, ln2_gain, ln2_bias).astype(jnp.bfloat16)
    pre_act = jnp.dot(normed_two, fc_weight, preferred_element_type=jnp.float32) + fc_bias
    hidden = jax.nn.gelu(pre_act, approximate=False).astype(jnp.bfloat16)
    return (middle_wide + jnp.dot(hidden, proj_weight, preferred_element_type=jnp.float32) + proj_bias).astype(jnp.bfloat16)


def reference(resid_in, grad_out, ln1_gain, ln1_bias, qkv_weight, qkv_bias, out_weight, out_bias,
              ln2_gain, ln2_bias, fc_weight, fc_bias, proj_weight, proj_bias):
    params = (ln1_gain, ln1_bias, qkv_weight, qkv_bias, out_weight, out_bias,
              ln2_gain, ln2_bias, fc_weight, fc_bias, proj_weight, proj_bias)

    def per_image(grad_sum, pair):
        tokens, cotangent = pair
        image_out, pullback = jax.vjp(layer_forward, params, tokens)
        param_grads, token_grad = pullback(cotangent)
        grad_sum = jax.tree.map(lambda total, fresh: total + fresh, grad_sum, param_grads)
        return grad_sum, (image_out, token_grad)

    start_sum = jax.tree.map(jnp.zeros_like, params)
    grad_sum, (resid_out, grad_in) = lax.scan(per_image, start_sum, (resid_in, grad_out))
    (grad_ln1_gain, grad_ln1_bias, grad_qkv_weight, grad_qkv_bias, grad_out_weight, grad_out_bias,
     grad_ln2_gain, grad_ln2_bias, grad_fc_weight, grad_fc_bias, grad_proj_weight, grad_proj_bias) = grad_sum
    return (resid_out, grad_in, grad_ln1_gain, grad_ln1_bias, grad_qkv_weight, grad_qkv_bias,
            grad_out_weight, grad_out_bias, grad_ln2_gain, grad_ln2_bias, grad_fc_weight, grad_fc_bias,
            grad_proj_weight, grad_proj_bias)
```

```python
import functools
import jax
import jax.numpy as jnp
from jax import lax
from jax.experimental import pallas as pl
from jax.experimental.pallas import tpu as pltpu
from jax.sharding import PartitionSpec as P

HEADS = 16
HEAD_DIM = 64
LN_EPS = 1e-5
LOG2E = 1.4426950408889634
CHUNKS = 2
AXIS = "fsdp"
NT = (((1,), (1,)), ((), ()))
TN = (((0,), (0,)), ((), ()))
NN = (((1,), (0,)), ((), ()))


def dot32(left, right, dims=NN):
    return lax.dot_general(left, right, dims, preferred_element_type=jnp.float32)


def params_of(parallel, mib=56):
    return pltpu.CompilerParams(dimension_semantics=("parallel" if parallel else "arbitrary",), vmem_limit_bytes=mib << 20)


def rows_spec(rows, cols):
    return pl.BlockSpec((rows, cols), lambda i: (i, 0))


def fixed_spec(*shape):
    return pl.BlockSpec(shape, lambda i: (0,) * len(shape))


def struct(shape, dtype):
    return jax.ShapeDtypeStruct(shape, dtype)


def normalize(values):
    mean_val = jnp.mean(values, axis=-1, keepdims=True)
    centered = values - mean_val
    inv_std = lax.rsqrt(jnp.mean(centered * centered, axis=-1, keepdims=True) + LN_EPS)
    return centered * inv_std, inv_std


def norm_kernel(x_ref, gain_ref, bias_ref, out_ref):
    hat, _ = normalize(x_ref[...].astype(jnp.float32))
    out_ref[...] = (hat * gain_ref[...] + bias_ref[...]).astype(jnp.bfloat16)


def norm_fwd(values, gain, bias, block):
    tokens, width = values.shape
    return pl.pallas_call(
        norm_kernel, grid=(tokens // block,),
        in_specs=[rows_spec(block, width), fixed_spec(1, width), fixed_spec(1, width)],
        out_specs=rows_spec(block, width), out_shape=struct((tokens, width), jnp.bfloat16),
        compiler_params=params_of(True),
        cost_estimate=pl.CostEstimate(flops=tokens * width * 400, bytes_accessed=tokens * width * 4, transcendentals=0),
        name="norm_fwd",
    )(values, gain, bias)


def norm_bwd_kernel(x_ref, dn_ref, gain_ref, resid_ref, *outs):
    grad_ref, low_ref, sums_ref = outs if len(outs) == 3 else (None,) + outs

    @pl.when(pl.program_id(0) == 0)
    def _():
        sums_ref[...] = jnp.zeros_like(sums_ref)

    hat, inv_std = normalize(x_ref[...].astype(jnp.float32))
    grad_norm = dn_ref[...]
    grad_hat = grad_norm * gain_ref[...]
    grad_vals = inv_std * (grad_hat - jnp.mean(grad_hat, axis=-1, keepdims=True)
                           - hat * jnp.mean(grad_hat * hat, axis=-1, keepdims=True))
    total = resid_ref[...].astype(jnp.float32) + grad_vals
    if grad_ref is not None:
        grad_ref[...] = total
    low_ref[...] = total.astype(jnp.bfloat16)
    sums_ref[0:1, :] += jnp.sum(grad_norm * hat, axis=0, keepdims=True)
    sums_ref[1:2, :] += jnp.sum(grad_norm, axis=0, keepdims=True)
    sums_ref[2:3, :] += jnp.sum(total, axis=0, keepdims=True)
    sums_ref[3:4, :] += jnp.sum(resid_ref[...].astype(jnp.float32), axis=0, keepdims=True)


def norm_bwd(values, grad_norm, gain, resid, keep_wide, block):
    tokens, width = values.shape
    wide = [(rows_spec(block, width), struct((tokens, width), jnp.float32))] if keep_wide else []
    outs = wide + [(rows_spec(block, width), struct((tokens, width), jnp.bfloat16)),
                   (fixed_spec(8, width), struct((8, width), jnp.float32))]
    return pl.pallas_call(
        norm_bwd_kernel, grid=(tokens // block,),
        in_specs=[rows_spec(block, width), rows_spec(block, width), fixed_spec(1, width), rows_spec(block, width)],
        out_specs=[spec for spec, _ in outs], out_shape=[shape for _, shape in outs],
        compiler_params=params_of(False),
        cost_estimate=pl.CostEstimate(flops=tokens * width * 800, bytes_accessed=tokens * width * 14, transcendentals=0),
        name="norm_bwd",
    )(values, grad_norm, gain, resid)


def pack_kernel(*refs):
    out_ref = refs[-1]
    out_ref[...] = jnp.zeros_like(out_ref)
    for n, ref in enumerate(refs[:-1]):
        out_ref[n:n + 1, 0:ref.shape[1]] = ref[...]


def pack_rows(vectors, rows):
    packed = pl.pallas_call(
        pack_kernel, out_shape=struct((rows, 128), jnp.float32), name="pack_rows",
    )(*[vector.reshape(1, -1) for vector in vectors])
    return packed.astype(jnp.bfloat16)


def attn_fwd_kernel(seq, qkv_ref, *refs):
    out_ref, lse_ref = refs[-2:]
    padded, width = out_ref.shape[1:]
    low = lax.broadcasted_iota(jnp.int32, (padded, 128), 1) < HEAD_DIM
    zero = jnp.zeros((padded, 128), jnp.bfloat16)
    scale = LOG2E * HEAD_DIM ** -0.5
    for pair in range(width // 128):
        cols = pl.ds(pair * 128, 128)
        query = qkv_ref[0, :, cols]
        key = qkv_ref[0, 0:seq, pl.ds(width + pair * 128, 128)]
        value = qkv_ref[0, 0:seq, pl.ds(2 * width + pair * 128, 128)]
        halves = []
        for side in range(2):
            own = jnp.where(low, query, zero) if side == 0 else jnp.where(low, zero, query)
            scores = dot32(key, own, NT)
            top = jnp.max(scores, axis=0, keepdims=True)
            powers = jnp.exp2((scores - top) * scale)
            total = jnp.sum(powers, axis=0, keepdims=True)
            lse_ref[0, pl.ds(2 * pair + side, 1), :] = top * scale + jnp.log2(total)
            halves.append(dot32((powers * (1.0 / total)).astype(jnp.bfloat16), value, TN))
        out_ref[0, :, cols] = jnp.where(low, halves[0], halves[1]).astype(jnp.bfloat16)


def attn_fwd(qkv, seq, chunk, earlier):
    images, padded, width3 = qkv.shape
    width = width3 // 3
    heads = width // HEAD_DIM
    extra = [] if earlier is None else [earlier]
    return pl.pallas_call(
        functools.partial(attn_fwd_kernel, seq), grid=(images,),
        in_specs=[pl.BlockSpec((1, padded, width3), lambda i: (i, 0, 0))] + [pl.BlockSpec(memory_space=pl.ANY)] * len(extra),
        out_specs=[pl.BlockSpec((1, padded, width), lambda i: (i, 0, chunk)), pl.BlockSpec((1, heads, padded), lambda i: (i, 0, 0))],
        out_shape=[struct((images, padded, width * CHUNKS), jnp.bfloat16), struct((images, heads, padded), jnp.float32)],
        input_output_aliases={1: 0} if extra else {},
        compiler_params=params_of(True),
        cost_estimate=pl.CostEstimate(flops=images * heads * seq * seq * 3000, bytes_accessed=images * seq * width * 8,
                                      transcendentals=images * heads * seq * seq),
        name="attn_fwd",
    )(qkv, *extra)


def attn_bwd_kernel(seq, qkv_ref, do_ref, lse_ref, grad_ref, sums_ref):
    padded, width = do_ref.shape[1:]
    low = lax.broadcasted_iota(jnp.int32, (padded, 128), 1) < HEAD_DIM
    zero = jnp.zeros((padded, 128), jnp.bfloat16)
    low_keys = lax.broadcasted_iota(jnp.int32, (seq, 128), 1) < HEAD_DIM
    scale = HEAD_DIM ** -0.5

    @pl.when(pl.program_id(0) == 0)
    def _():
        sums_ref[...] = jnp.zeros_like(sums_ref)

    grad_ref[0, seq:, :] = jnp.zeros((padded - seq, 3 * width), jnp.bfloat16)
    for pair in range(width // 128):
        cols = pl.ds(pair * 128, 128)
        key_cols = pl.ds(width + pair * 128, 128)
        value_cols = pl.ds(2 * width + pair * 128, 128)
        query = qkv_ref[0, :, cols]
        key = qkv_ref[0, 0:seq, key_cols]
        value = qkv_ref[0, 0:seq, value_cols]
        grad_out = do_ref[0, :, cols]
        grads_q, grads_k, grads_v = [], [], []
        for side in range(2):
            def own(array):
                return jnp.where(low, array, zero) if side == 0 else jnp.where(low, zero, array)
            scores = dot32(key, own(query), NT)
            probs = jnp.exp2(scores * (scale * LOG2E) - lse_ref[0, pl.ds(2 * pair + side, 1), :])
            grad_probs = dot32(value, own(grad_out), NT)
            inner = jnp.sum(grad_probs * probs, axis=0, keepdims=True)
            grad_scores = (probs * (grad_probs - inner) * scale).astype(jnp.bfloat16)
            grads_v.append(dot32(probs.astype(jnp.bfloat16), grad_out))
            grads_k.append(dot32(grad_scores, query))
            grads_q.append(dot32(grad_scores, key, TN))
        grad_q = jnp.where(low, grads_q[0], grads_q[1])
        grad_ref[0, :, cols] = grad_q.astype(jnp.bfloat16)
        sums_ref[0:1, cols] += jnp.sum(grad_q, axis=0, keepdims=True)
        for where, halves in ((key_cols, grads_k), (value_cols, grads_v)):
            both = jnp.where(low_keys, halves[0], halves[1])
            grad_ref[0, 0:seq, where] = both.astype(jnp.bfloat16)
            sums_ref[0:1, where] += jnp.sum(both, axis=0, keepdims=True)


def attn_bwd(qkv, grad_out, lse, seq, chunk):
    images, padded, width3 = qkv.shape
    width = width3 // 3
    heads = width // HEAD_DIM
    return pl.pallas_call(
        functools.partial(attn_bwd_kernel, seq), grid=(images,),
        in_specs=[pl.BlockSpec((1, padded, width3), lambda i: (i, 0, 0)),
                  pl.BlockSpec((1, padded, width), lambda i: (i, 0, chunk)),
                  pl.BlockSpec((1, heads, padded), lambda i: (i, 0, 0))],
        out_specs=[pl.BlockSpec((1, padded, width3), lambda i: (i, 0, 0)), fixed_spec(8, width3)],
        out_shape=[struct((images, padded, width3), jnp.bfloat16), struct((8, width3), jnp.float32)],
        compiler_params=params_of(False),
        cost_estimate=pl.CostEstimate(flops=images * heads * seq * seq * 6000, bytes_accessed=images * seq * width * 16,
                                      transcendentals=images * heads * seq * seq),
        name="attn_bwd",
    )(qkv, grad_out, lse)


def fc_kernel(step, x_ref, w_ref, bias_ref, hidden_ref, slope_ref):
    rows = x_ref[...]
    for start in range(0, w_ref.shape[1], step):
        cols = pl.ds(start, step)
        pre = dot32(rows, w_ref[:, cols]) + bias_ref[:, cols]
        cdf = 0.5 * (1.0 + lax.erf(pre * (0.5 ** 0.5)))
        pdf = jnp.exp(-0.5 * pre * pre) * 0.3989422804014327
        hidden_ref[:, cols] = (pre * cdf).astype(jnp.bfloat16)
        slope_ref[:, cols] = cdf + pre * pdf


def fc_fwd(normed, weight, bias, block):
    tokens, width = normed.shape
    ffn = weight.shape[1]
    return pl.pallas_call(
        functools.partial(fc_kernel, 512), grid=(tokens // block,),
        in_specs=[rows_spec(block, width), fixed_spec(width, ffn), fixed_spec(1, ffn)],
        out_specs=[rows_spec(block, ffn), rows_spec(block, ffn)],
        out_shape=[struct((tokens, ffn), jnp.bfloat16), struct((tokens, ffn), jnp.float32)],
        compiler_params=params_of(True),
        cost_estimate=pl.CostEstimate(flops=2 * tokens * width * ffn, bytes_accessed=tokens * ffn * 6, transcendentals=tokens * ffn),
        name="fc_fwd",
    )(normed, weight, bias)


def fc_bwd_kernel(step, dy_ref, w_ref, slope_ref, grad_ref, sums_ref):
    @pl.when(pl.program_id(0) == 0)
    def _():
        sums_ref[...] = jnp.zeros_like(sums_ref)

    rows = dy_ref[...]
    for start in range(0, w_ref.shape[0], step):
        cols = pl.ds(start, step)
        grad = dot32(rows, w_ref[cols, :], NT) * slope_ref[:, cols]
        grad_ref[:, cols] = grad.astype(jnp.bfloat16)
        sums_ref[0:1, cols] += jnp.sum(grad, axis=0, keepdims=True)


def fc_bwd(grad_out, weight, slope, block):
    tokens, width = grad_out.shape
    ffn = weight.shape[0]
    return pl.pallas_call(
        functools.partial(fc_bwd_kernel, 512), grid=(tokens // block,),
        in_specs=[rows_spec(block, width), fixed_spec(ffn, width), rows_spec(block, ffn)],
        out_specs=[rows_spec(block, ffn), fixed_spec(8, ffn)],
        out_shape=[struct((tokens, ffn), jnp.bfloat16), struct((8, ffn), jnp.float32)],
        compiler_params=params_of(False),
        cost_estimate=pl.CostEstimate(flops=2 * tokens * width * ffn, bytes_accessed=tokens * ffn * 6, transcendentals=0),
        name="fc_bwd",
    )(grad_out, weight, slope)


def exchange(values, bit, devices):
    return lax.ppermute(values, AXIS, [(i, i ^ (1 << bit)) for i in range(devices)])


def my_bit(bit):
    return (lax.axis_index(AXIS) >> bit) & 1


class ScatterPart:
    def __init__(self, terms, done, order, devices, cols):
        self.terms, self.done, self.order = list(terms), list(done), list(order)
        self.devices, self.cols = devices, cols
        self.left = [bit for bit in range(devices.bit_length() - 2, -1, -1) if bit not in done]
        self.got = self.sent = None

    def total(self, bit=None):
        chosen = {known: my_bit(known) for known in self.done}
        if bit is not None:
            chosen[bit] = 1 - my_bit(bit)
        out = []
        for array, bits, start in self.terms:
            rows = array.shape[-2]
            starts = [chosen.get(known, 0) for known in bits] + [0, start]
            sizes = [1 if known in chosen else 2 for known in bits] + [rows, self.cols]
            kept = [2 for known in bits if known not in chosen]
            out.append(lax.dynamic_slice(array, starts, sizes).reshape(kept + [rows, self.cols]))
        return functools.reduce(jnp.add, out)

    def take(self):
        if self.got is not None:
            self.terms.append((self.got, list(self.left), 0))
            self.got = None

    def prepare(self):
        self.take()
        self.bit = self.order.pop(0)
        self.sent = self.total(self.bit)
        self.left.remove(self.bit)

    def launch(self):
        self.got = exchange(self.sent, self.bit, self.devices)
        self.done.append(self.bit)
        self.sent = None

    def result(self):
        self.take()
        return self.total()


class Scatter:
    def __init__(self, grad, devices, split=True):
        bits = devices.bit_length() - 1
        rows, cols = grad.shape
        view = grad.reshape((2,) * bits + (rows // devices, cols))
        self.devices, self.split = devices, split
        self.parts = [ScatterPart([(view, list(range(bits - 1, -1, -1)), 0)], [], [0] if split else list(range(bits)), devices, cols)]

    def prepare(self):
        whole = self.parts[0]
        if self.split and not whole.order:
            whole.take()
            half = whole.cols // 2
            rest = list(range(3, self.devices.bit_length() - 1))
            self.parts = [ScatterPart([(array, bits, half * n) for array, bits, _ in whole.terms], whole.done, order + rest, self.devices, half)
                          for n, order in enumerate(([1, 2], [2, 1]))]
            self.split = False
        for part in self.parts:
            part.prepare()

    def result(self):
        results = [part.result() for part in self.parts]
        return results[0] if len(results) == 1 else jnp.concatenate(results, axis=1)


def advance(value, *chains):
    arrived = [part.got for chain in chains for part in chain.parts]
    held = [got for got in arrived if got is not None]
    value, held = lax.optimization_barrier((value, held))
    held = iter(held)
    for chain in chains:
        for part in chain.parts:
            if part.got is not None:
                part.got = next(held)
        chain.prepare()
    parts = [part for chain in chains for part in chain.parts]
    value, sent = lax.optimization_barrier((value, [part.sent for part in parts]))
    for part, array in zip(parts, sent):
        part.sent = array
        part.launch()
    return value


class GatherPart:
    def __init__(self, shard, order, devices):
        self.sent, self.got = shard, None
        self.order, self.have, self.devices = list(order), [], devices

    def prepare(self):
        self.take()
        self.bit = self.order.pop(0)

    def launch(self):
        self.got = exchange(self.sent, self.bit, self.devices)

    def take(self):
        if self.got is None:
            return
        axis = sum(bit > self.bit for bit in self.have)
        mine = my_bit(self.bit) == 0
        self.sent = jnp.stack([jnp.where(mine, self.sent, self.got), jnp.where(mine, self.got, self.sent)], axis=axis)
        self.have = sorted(self.have + [self.bit], reverse=True)
        self.got = None


class Gather:
    def __init__(self, shard, devices):
        bits = devices.bit_length() - 1
        half = shard.shape[1] // 2
        rest = list(range(bits - 1, 2, -1))
        self.parts = [GatherPart(shard[:, :half], rest + [2, 1, 0], devices), GatherPart(shard[:, half:], rest + [1, 2, 0], devices)]

    def prepare(self):
        for part in self.parts:
            part.prepare()

    def result(self):
        for part in self.parts:
            part.take()
        full = jnp.concatenate([part.sent for part in self.parts], axis=-1)
        return full.reshape(-1, full.shape[-1])


def gather(shard):
    return lax.all_gather(shard, AXIS, axis=0, tiled=True)


def solution(mesh):
    specs = (P(AXIS),) * 14
    devices = mesh.shape[AXIS]

    def device_step(resid_in, grad_out, *shards):
        (ln1_gain, ln1_bias, qkv_weight, qkv_bias, out_weight, out_bias,
         ln2_gain, ln2_bias, fc_weight, fc_bias, proj_weight, proj_bias) = shards
        images, seq, width = resid_in.shape
        padded = -(-seq // 8) * 8
        block = padded
        tokens = images * padded
        part = width // CHUNKS
        vectors = (ln1_gain, ln1_bias, qkv_bias, out_bias, ln2_gain, ln2_bias, fc_bias, proj_bias)
        sizes = [vector.shape[0] for vector in vectors]
        per_row = qkv_weight.shape[0]

        def flat(array):
            return jnp.pad(array, ((0, 0), (0, padded - seq), (0, 0))).reshape(tokens, width)

        def to_chunks(array):
            split = array.reshape(array.shape[:-1] + (3, CHUNKS, part))
            return [split[..., :, n, :].reshape(array.shape[:-1] + (3 * part,)) for n in range(CHUNKS)]

        def from_chunks(chunks):
            split = [chunk.reshape(chunk.shape[:-1] + (3, part)) for chunk in chunks]
            return jnp.stack(split, axis=-2).reshape(chunks[0].shape[:-1] + (3 * width,))

        small = pack_rows(vectors, per_row)
        qkv_shards = to_chunks(qkv_weight.astype(jnp.bfloat16))
        chains = [Gather(jnp.concatenate([qkv_shards[0], small], axis=1), devices), Gather(qkv_shards[1], devices), Gather(out_weight.astype(jnp.bfloat16), devices)]
        fc_full, proj_full = gather(fc_weight.astype(jnp.bfloat16)), gather(proj_weight.astype(jnp.bfloat16))
        steps = devices.bit_length() - 1
        resid = flat(resid_in)
        grad_y = flat(grad_out)
        advance(None, chains[0])
        resid = advance(resid, chains[0])
        resid, grad_y = advance((resid, grad_y), chains[0])
        for _ in range(steps - 3):
            resid = advance(resid, chains[0])
        first = chains[0].result()
        small_full = first[:, 3 * part:].reshape(devices, per_row, 128)[:, :len(sizes)].astype(jnp.float32)
        (ln1_gain, ln1_bias, qkv_bias, out_bias, ln2_gain, ln2_bias, fc_bias, proj_bias) = [
            small_full[:, n, :size].reshape(1, devices * size) for n, size in enumerate(sizes)]

        normed_one = norm_fwd(resid, ln1_gain, ln1_bias, block)
        normed_one = advance(normed_one, chains[1])
        qkv_biases = to_chunks(qkv_bias)
        qkv_full, qkv_vals, lses, mixed = [first[:, :3 * part]], [], [], None
        vals = (dot32(normed_one, qkv_full[0]) + qkv_biases[0]).astype(jnp.bfloat16).reshape(images, padded, 3 * part)
        vals = advance(vals, chains[1])
        mixed, lse = attn_fwd(vals, seq, 0, mixed)
        qkv_vals.append(vals)
        lses.append(lse)
        for _ in range(steps - 2):
            mixed = advance(mixed, chains[1], chains[2])
        qkv_full.append(chains[1].result())
        vals = (dot32(normed_one, qkv_full[1]) + qkv_biases[1]).astype(jnp.bfloat16).reshape(images, padded, 3 * part)
        vals = advance(vals, chains[2])
        mixed, lse = attn_fwd(vals, seq, 1, mixed)
        qkv_vals.append(vals)
        lses.append(lse)
        mixed = advance(mixed, chains[2])
        out_full = chains[2].result()
        mixed = mixed.reshape(tokens, width)
        middle = (resid.astype(jnp.float32) + dot32(mixed, out_full) + out_bias).astype(jnp.bfloat16)
        normed_two = norm_fwd(middle, ln2_gain, ln2_bias, block)
        hidden, slope = fc_fwd(normed_two, fc_full, fc_bias, block)

        of_proj = Scatter(dot32(hidden, grad_y, TN), devices)
        grad_y = advance(grad_y, of_proj)
        grad_pre, fc_sums = fc_bwd(grad_y, proj_full, slope, block)
        grad_pre = advance(grad_pre, of_proj)
        of_fc = Scatter(dot32(normed_two, grad_pre, TN), devices)
        grad_pre = advance(grad_pre, of_fc)
        grad_norm = dot32(grad_pre, fc_full, NT)
        grad_norm = advance(grad_norm, of_proj, of_fc)
        grad_mid, grad_mid_low, sums_two = norm_bwd(middle, grad_norm, ln2_gain, grad_y, True, block)
        d_out = lax.psum_scatter(dot32(mixed, grad_mid_low, TN), AXIS, scatter_dimension=0, tiled=True)
        grad_mixed = dot32(grad_mid_low, out_full, NT).astype(jnp.bfloat16).reshape(images, padded, width)
        of_qkv, qkv_sums = [], []
        vals_one, sums = attn_bwd(qkv_vals[0], grad_mixed, lses[0], seq, 0)
        qkv_sums.append(sums[0:1])
        vals_one = advance(vals_one.reshape(tokens, 3 * part), of_proj)
        of_qkv.append(Scatter(dot32(normed_one, vals_one, TN), devices))
        grad_mixed, vals_one = advance((grad_mixed, vals_one), of_qkv[0], of_fc)
        vals_two, sums = attn_bwd(qkv_vals[1], grad_mixed, lses[1], seq, 1)
        qkv_sums.append(sums[0:1])
        vals_two = advance(vals_two.reshape(tokens, 3 * part), of_proj, of_fc, of_qkv[0])
        of_qkv.append(Scatter(dot32(normed_one, vals_two, TN), devices))
        vals_one, vals_two = advance((vals_one, vals_two), of_qkv[1])
        grad_norm = dot32(vals_one, qkv_full[0], NT)
        grad_norm, vals_two = advance((grad_norm, vals_two), of_qkv[1], of_qkv[0])
        grad_norm = grad_norm + dot32(vals_two, qkv_full[1], NT)
        grad_norm = advance(grad_norm, of_qkv[0], of_fc)
        grad_in, sums_one = norm_bwd(resid, grad_norm, ln1_gain, grad_mid, False, block)

        vector_grads = (sums_one[0], sums_one[1], from_chunks(qkv_sums)[0], sums_two[2], sums_two[0], sums_two[1], fc_sums[0], sums_two[3])
        packed = jnp.stack([jnp.pad(grad.reshape(devices, size), ((0, 0), (0, 128 - size))) for grad, size in zip(vector_grads, sizes)], axis=1)
        packed = packed.reshape(devices * len(sizes), 128)
        packed = Scatter(packed, devices, split=False)
        hidden = advance(hidden, of_qkv[1], of_qkv[0], packed)

        def last(rows):
            return (middle[rows].astype(jnp.float32) + dot32(hidden[rows], proj_full) + proj_bias).astype(jnp.bfloat16)

        cut = tokens // 2
        upper = last(slice(0, cut))
        hidden, upper = advance((hidden, upper), of_qkv[1], packed)
        lower = last(slice(cut, tokens))
        lower = advance(lower, of_qkv[1], packed)
        resid_out = jnp.concatenate([upper, lower])

        def unflat(array):
            return array.reshape(images, padded, width)[:, :seq]

        resid_out = advance(unflat(resid_out), packed)
        grad_in = advance(unflat(grad_in), packed)
        packed = packed.result()
        (d_ln1_gain, d_ln1_bias, d_qkv_bias, d_out_bias, d_ln2_gain, d_ln2_bias, d_fc_bias, d_proj_bias) = [
            packed[n, :size] for n, size in enumerate(sizes)]
        d_qkv = from_chunks([chain.result() for chain in of_qkv])
        return (resid_out, grad_in, d_ln1_gain, d_ln1_bias, d_qkv, d_qkv_bias, d_out, d_out_bias,
                d_ln2_gain, d_ln2_bias, of_fc.result(), d_fc_bias, of_proj.result(), d_proj_bias)

    return jax.shard_map(device_step, mesh=mesh, in_specs=specs, out_specs=specs, check_vma=False)
```
